256 devices in a mesh: grp: 16 (over y, z_hi, core), dp: 16 (over z_lo, x).
Axes of the slice: x: 4, y: 4, z: 8 (z_hi: 2, z_lo: 4; z = z_hi * 4 + z_lo), core: 2. Of those that a mesh axis runs over, the one named last changes fastest.
Arguments:
- tokens: bfloat16 [16, 2048, 2048], P('grp', 'dp'), may hold values from -6 to 6
- hidden_grad: bfloat16 [16, 2048, 6144], P('grp', 'dp'), may hold values from -6 to 6
- w_gate: bfloat16 [16, 2048, 6144], P('grp', None, 'dp'), may hold values from -6 to 6
- w_up: bfloat16 [16, 2048, 6144], P('grp', None, 'dp'), may hold values from -6 to 6
Outputs:
- mixed_gate: bfloat16 [16, 2048, 6144], P('grp', None, 'dp')
- mixed_up: bfloat16 [16, 2048, 6144], P('grp', None, 'dp')
The draws below stay inside these ranges and needn't reach their ends.
All inputs are finite; a program needn't handle non-finite values.
Results may differ from the reference program's by a relative error of at most 0.0052.
Values may be sent and summed in bfloat16 or wider, within the bound.
A program may use at most 256 MiB of HBM per device.

```python
import jax
import jax.numpy as jnp
from jax import lax

D = 2048
FF = 6144
GROUPS = 16
GROUP_TOKENS = 2048


def level_of(rng, shape, cuts, smallest, high):
    def one(axis_at, parts):
        heights = jax.random.uniform(jax.random.fold_in(jax.random.fold_in(rng, 6), axis_at), (parts,), jnp.float32, smallest / len(cuts), high / len(cuts))
        return jnp.repeat(jnp.exp(heights), shape[axis_at] // parts).reshape((-1,) + (1,) * (len(shape) - axis_at - 1))

    loudness = one(*cuts[0])
    for cut in cuts[1:]:
        loudness = loudness * one(*cut)
    return loudness


def scatter_about(key, dims, spread, reach, cuts=(), kind=jnp.bfloat16):
    drawn = jax.random.normal(key, dims, jnp.float32) * spread
    if len(cuts) > 0:
        drawn = level_of(key, dims, cuts, -0.22, 0.18) * drawn
    return jnp.clip(drawn, min=-reach, max=reach).astype(kind)


def setup_inputs(seed: int = 0) -> dict:
    key_of = jax.random.split(jax.random.key(seed), 5)
    tokens = scatter_about(key_of[0], (GROUPS, GROUP_TOKENS, D), 1.0, 6.0, ((0, 16), (1, 16)))
    hidden_grad = scatter_about(key_of[1], (GROUPS, GROUP_TOKENS, FF), 1.0, 6.0, ((0, 16), (1, 16)))
    w_gate = scatter_about(key_of[2], (GROUPS, D, FF), 1.0, 6.0, ((0, 16), (2, 16)))
    w_up = scatter_about(key_of[3], (GROUPS, D, FF), 1.0, 6.0, ((0, 16), (2, 16)))
    return dict(tokens=tokens, hidden_grad=hidden_grad, w_gate=w_gate, w_up=w_up)


def one_replica(operands):
    rows, cotangent, gate_weight, up_weight = operands
    scale = D ** -0.5
    gate = jnp.dot(rows, gate_weight, preferred_element_type=jnp.float32) * scale
    up = jnp.dot(rows, up_weight, preferred_element_type=jnp.float32) * scale
    sigma = jax.nn.sigmoid(gate)
    upstream = cotangent.astype(jnp.float32)
    gate_rows = (upstream * up * sigma * (1.0 + gate * (1.0 - sigma))).astype(jnp.bfloat16)
    up_rows = (upstream * gate * sigma).astype(jnp.bfloat16)
    gate_grad = jnp.dot(rows.T, gate_rows, preferred_element_type=jnp.float32) * scale
    up_grad = jnp.dot(rows.T, up_rows, preferred_element_type=jnp.float32) * scale
    gate_step = (gate_weight.astype(jnp.float32) - 0.5 * gate_grad).astype(jnp.bfloat16)
    up_step = (up_weight.astype(jnp.float32) - 0.5 * up_grad).astype(jnp.bfloat16)
    return gate_step, up_step


def average_cycle(stepped):
    wide = stepped.astype(jnp.float32)
    mixed = 0.5 * wide + 0.25 * (jnp.roll(wide, 1, axis=0) + jnp.roll(wide, -1, axis=0))
    return mixed.astype(jnp.bfloat16)


def reference(tokens, hidden_grad, w_gate, w_up):
    gate_step, up_step = lax.map(one_replica, (tokens, hidden_grad, w_gate, w_up))
    return average_cycle(gate_step), average_cycle(up_step)
```

```python
import functools

import jax
import jax.numpy as jnp
from jax import lax
from jax.experimental import pallas as pl
from jax.experimental.pallas import tpu as pltpu
from jax.sharding import PartitionSpec as P

MESH = pl.DeviceIdType.MESH
LINE = 4
STAGGER = True


def kernel(
    groups, tokens, hidden_grad, w_gate, w_up, out_gate, out_up,
    tok, cot, wts, rows, acc, grad, step, from_twin, from_far,
    load_sem, own_sem,
    z_send, z_recv, x_send, x_recv, half_send, half_recv,
    cot_send, cot_recv, step_send, step_recv, out_sem, turn,
):
    width = tok.shape[1]
    scale = width ** (-0.5)
    shard = tokens.shape[1]
    units = w_gate.shape[2]
    chunk = LINE * shard
    tall = 256
    blocks = width // tall

    g = lax.axis_index("grp")
    d = lax.axis_index("dp")
    z, x = d // LINE, d % LINE
    core = g % 2
    even = core == 0
    odd = core == 1
    twin = g + 1 - 2 * core
    far = (g - 1 + 2 * core + groups) % groups
    x_left, x_right, x_opp = (x + 3) % LINE, (x + 1) % LINE, (x + 2) % LINE

    def row_of(k):
        flip = z // 2
        low = z + flip * (3 - 2 * z)
        near = (1 - k // 2) * ((low + k) % 2) + (k // 2) * k
        return near + flip * (3 - 2 * near)

    barrier = pltpu.get_barrier_semaphore()

    def greet(i, carry):
        peer = (d + i) % 16
        pl.semaphore_signal(barrier, inc=1, device_id=(g, peer), device_id_type=MESH)
        return carry

    lax.fori_loop(1, 16, greet, 0)
    pl.semaphore_signal(barrier, inc=1, device_id=(twin, d), device_id_type=MESH)
    pl.semaphore_signal(barrier, inc=1, device_id=(far, d), device_id_type=MESH)

    def shard_at(row, col):
        return pl.ds(pl.multiple_of((row * LINE + col) * shard, shard), shard)

    loads = [
        pltpu.make_async_copy(tokens.at[0], tok.at[shard_at(z, x)], own_sem),
        pltpu.make_async_copy(w_gate.at[0], wts.at[:, pl.ds(0, units)], load_sem.at[0]),
        pltpu.make_async_copy(w_up.at[0], wts.at[:, pl.ds(units, units)], load_sem.at[1]),
        pltpu.make_async_copy(
            hidden_grad.at[0, :, pl.ds(pl.multiple_of(d * units, 128), units)],
            cot.at[shard_at(z, x)],
            load_sem.at[2],
        ),
    ]
    for load in loads:
        load.start()
    grad[...] = jnp.zeros_like(grad)
    loads[0].wait()
    pl.semaphore_wait(barrier, 17)

    def z_copy(row, way, to):
        return pltpu.make_async_remote_copy(
            src_ref=tok.at[shard_at(row, x)],
            dst_ref=tok.at[shard_at(row, x)],
            send_sem=z_send.at[way, row],
            recv_sem=z_recv.at[row],
            device_id=(g, to * LINE + x),
            device_id_type=MESH,
        )

    def x_copy(row, col, way):
        to = x_right if way == 0 else x_left
        return pltpu.make_async_remote_copy(
            src_ref=tok.at[shard_at(row, col)],
            dst_ref=tok.at[shard_at(row, col)],
            send_sem=x_send.at[way, row],
            recv_sem=x_recv.at[way, row],
            device_id=(g, z * LINE + to),
            device_id_type=MESH,
        )

    def half_copy(row, col, way):
        half = shard // 2
        at = pl.ds(pl.multiple_of((row * LINE + col) * shard + way * half, half), half)
        to = x_right if way == 0 else x_left
        return pltpu.make_async_remote_copy(
            src_ref=tok.at[at],
            dst_ref=tok.at[at],
            send_sem=half_send.at[way, row],
            recv_sem=half_recv.at[way, row],
            device_id=(g, z * LINE + to),
            device_id_type=MESH,
        )

    def send_z(row):
        @pl.when((z < LINE - 1) & (row <= z))
        def _():
            z_copy(row, 0, z + 1).start()

        @pl.when((z > 0) & (row >= z))
        def _():
            z_copy(row, 1, z - 1).start()

    def take_z(row):
        z_copy(row, 0, z).wait_recv()
        send_z(row)

    def send_x(row):
        x_copy(row, x, 0).start()
        x_copy(row, x, 1).start()

    def relay_x(row):
        x_copy(row, x_left, 0).wait_recv()
        half_copy(row, x_left, 0).start()
        x_copy(row, x_right, 1).wait_recv()
        half_copy(row, x_right, 1).start()

    def cot_copy(i):
        peer = (d + i) % 16
        return pltpu.make_async_remote_copy(
            src_ref=hidden_grad.at[0, :, pl.ds(pl.multiple_of(peer * units, 128), units)],
            dst_ref=cot.at[shard_at(z, x)],
            send_sem=cot_send.at[i],
            recv_sem=cot_recv.at[d],
            device_id=(g, peer),
            device_id_type=MESH,
        )

    def take_cot(source):
        pltpu.make_async_remote_copy(
            src_ref=cot.at[pl.ds(pl.multiple_of(source * shard, shard), shard)],
            dst_ref=cot.at[pl.ds(pl.multiple_of(source * shard, shard), shard)],
            send_sem=cot_send.at[0],
            recv_sem=cot_recv.at[source],
            device_id=(g, source),
            device_id_type=MESH,
        ).wait_recv()

    def gating(row):
        for col in (x_left, x_right, x_opp):
            take_cot(row * LINE + col)

        @pl.when(row != z)
        def _():
            take_cot(row * LINE + x)

        def part(m, carry):
            at = pl.ds(pl.multiple_of(row * chunk + m * tall, tall), tall)
            acc[...] = jnp.dot(tok[at, :], wts[...], preferred_element_type=jnp.float32)
            gate = acc[:, :units] * scale
            up = acc[:, units:] * scale
            sigma = jax.nn.sigmoid(gate)
            upstream = cot[at, :].astype(jnp.float32)
            to = pl.ds(pl.multiple_of(m * tall, tall), tall)
            rows[to, :units] = (upstream * up * sigma * (1.0 + gate * (1.0 - sigma))).astype(jnp.bfloat16)
            rows[to, units:] = (upstream * gate * sigma).astype(jnp.bfloat16)
            return carry

        lax.fori_loop(0, chunk // tall, part, 0)

    def gradient(row, b):
        at = pl.ds(pl.multiple_of(row * chunk, chunk), chunk)
        to = pl.ds(pl.multiple_of(b * tall, tall), tall)
        return grad[to, :] + lax.dot_general(
            tok[at, to], rows[...], (((0,), (0,)), ((), ())), preferred_element_type=jnp.float32
        )

    def finish_row(row):
        half_copy(row, x_opp, 0).wait_recv()
        half_copy(row, x_opp, 1).wait_recv()
        gating(row)

    def middle(row):
        finish_row(row)

        def block(b, carry):
            to = pl.ds(pl.multiple_of(b * tall, tall), tall)
            grad[to, :] = gradient(row, b)
            return carry

        lax.fori_loop(0, blocks, block, 0)

    if STAGGER:
        @pl.when(odd)
        def _():
            pl.semaphore_wait(turn.at[0], 1)

    send_z(z)
    if STAGGER:
        @pl.when(even)
        def _():
            send_x(z)
    else:
        send_x(z)

    def exchange(i, carry):
        cot_copy(i).start()
        return carry

    lax.fori_loop(1, 16, exchange, 0)
    for load in loads[1:]:
        load.wait()

    def my_turn(i):
        pl.semaphore_signal(turn.at[i], inc=1, device_id=(twin, d), device_id_type=MESH)

    if STAGGER:
        @pl.when(odd)
        def _():
            for k in range(1, LINE):
                take_z(row_of(k))
            pl.semaphore_wait(turn.at[1], 1)
            send_x(z)

    def stage(k, carry):
        @pl.when(k < LINE - 1)
        def _():
            row = row_of(k + 1)
            if STAGGER:
                @pl.when(even)
                def _():
                    take_z(row)
            else:
                take_z(row)
            send_x(row)

        if STAGGER:
            @pl.when(even & (k == 2))
            def _():
                my_turn(0)

        relay_x(row_of(k))

        if STAGGER:
            @pl.when(even & (k == 3))
            def _():
                my_turn(1)

        @pl.when(k > 0)
        def _():
            middle(row_of(k - 1))

        return carry

    lax.fori_loop(0, LINE, stage, 0)

    last = row_of(LINE - 1)
    finish_row(last)

    def step_copy(b, way):
        to = pl.ds(pl.multiple_of(b * tall, tall), tall)
        return pltpu.make_async_remote_copy(
            src_ref=step.at[to],
            dst_ref=(from_twin if way == 0 else from_far).at[to],
            send_sem=step_send.at[way, b],
            recv_sem=step_recv.at[way, b],
            device_id=((twin if way == 0 else far), d),
            device_id_type=MESH,
        )

    def send_step(b):
        step_copy(b, 1).start()
        step_copy(b, 0).start()

    def final(b, carry):
        to = pl.ds(pl.multiple_of(b * tall, tall), tall)
        moved = wts[to, :].astype(jnp.float32) - 0.5 * (gradient(last, b) * scale)
        step[to, :] = moved.astype(jnp.bfloat16)

        @pl.when(b > 0)
        def _():
            send_step(b - 1)

        return carry

    lax.fori_loop(0, blocks, final, 0)
    send_step(blocks - 1)

    def out_copies(b):
        to = pl.ds(pl.multiple_of(b * tall, tall), tall)
        return (
            pltpu.make_async_copy(from_far.at[to, pl.ds(0, units)], out_gate.at[0, to], out_sem.at[0, b]),
            pltpu.make_async_copy(from_far.at[to, pl.ds(units, units)], out_up.at[0, to], out_sem.at[1, b]),
        )

    def mix(b, carry):
        to = pl.ds(pl.multiple_of(b * tall, tall), tall)
        step_copy(b, 0).wait_recv()
        step_copy(b, 1).wait_recv()
        mixed = 0.5 * step[to, :].astype(jnp.float32) + 0.25 * (
            from_twin[to, :].astype(jnp.float32) + from_far[to, :].astype(jnp.float32)
        )
        from_far[to, :] = mixed.astype(jnp.bfloat16)
        for copy in out_copies(b):
            copy.start()
        return carry

    lax.fori_loop(0, blocks, mix, 0)

    def sent_rows(k, carry):
        row = row_of(k)
        @pl.when((z < LINE - 1) & (row <= z))
        def _():
            z_copy(row, 0, z + 1).wait_send()

        @pl.when((z > 0) & (row >= z))
        def _():
            z_copy(row, 1, z - 1).wait_send()

        x_copy(row, x, 0).wait_send()
        x_copy(row, x, 1).wait_send()
        half_copy(row, x_left, 0).wait_send()
        half_copy(row, x_right, 1).wait_send()
        return carry

    lax.fori_loop(0, LINE, sent_rows, 0)

    def sent_cot(i, carry):
        cot_copy(i).wait_send()
        return carry

    lax.fori_loop(1, 16, sent_cot, 0)

    def sent_blocks(b, carry):
        step_copy(b, 0).wait_send()
        step_copy(b, 1).wait_send()
        for copy in out_copies(b):
            copy.wait()
        return carry

    lax.fori_loop(0, blocks, sent_blocks, 0)


def solution(mesh):
    groups = mesh.shape["grp"]

    def local(tokens, hidden_grad, w_gate, w_up):
        shard, width = tokens.shape[1:]
        units = w_gate.shape[2]
        count = shard * mesh.shape["dp"]
        chunk = LINE * shard
        tall = 256
        blocks = width // tall
        dma = pltpu.SemaphoreType.DMA
        out = jax.ShapeDtypeStruct(w_gate.shape, jnp.bfloat16)
        wide = 2 * units
        return pl.pallas_call(
            functools.partial(kernel, groups),
            out_shape=(out, out),
            in_specs=[pl.BlockSpec(memory_space=pl.ANY)] * 4,
            out_specs=(pl.BlockSpec(memory_space=pl.ANY),) * 2,
            scratch_shapes=[
                pltpu.VMEM((count, width), jnp.bfloat16),
                pltpu.VMEM((count, units), jnp.bfloat16),
                pltpu.VMEM((width, wide), jnp.bfloat16),
                pltpu.VMEM((chunk, wide), jnp.bfloat16),
                pltpu.VMEM((tall, wide), jnp.float32),
                pltpu.VMEM((width, wide), jnp.float32),
                pltpu.VMEM((width, wide), jnp.bfloat16),
                pltpu.VMEM((width, wide), jnp.bfloat16),
                pltpu.VMEM((width, wide), jnp.bfloat16),
                dma((3,)),
                dma(()),
                dma((2, LINE)),
                dma((LINE,)),
                dma((2, LINE)),
                dma((2, LINE)),
                dma((2, LINE)),
                dma((2, LINE)),
                dma((16,)),
                dma((16,)),
                dma((2, blocks)),
                dma((2, blocks)),
                dma((2, blocks)),
                pltpu.SemaphoreType.REGULAR((2,)),
            ],
            compiler_params=pltpu.CompilerParams(
                collective_id=0, has_side_effects=True, vmem_limit_bytes=60 * 1024 * 1024
            ),
        )(tokens, hidden_grad, w_gate, w_up)

    in_specs = (
        P("grp", "dp", None),
        P("grp", "dp", None),
        P("grp", None, "dp"),
        P("grp", None, "dp"),
    )
    out_specs = (P("grp", None, "dp"), P("grp", None, "dp"))
    return jax.shard_map(local, mesh=mesh, in_specs=in_specs, out_specs=out_specs, check_vma=False)
```

```python
import functools

import jax
import jax.numpy as jnp
from jax import lax
from jax.experimental import pallas as pl
from jax.experimental.pallas import tpu as pltpu
from jax.sharding import PartitionSpec as P

MESH = pl.DeviceIdType.MESH
LINE = 4
PIECES = 2
TURN_Z = 2
INNER_AT = 1
OUTER_AT = 2
EARLY_ROWS = 1
OUTER_ODD = 0


def kernel(
    groups, tokens, hidden_grad, w_gate, w_up, out,
    tok, cot, wts, rows, acc, step, from_twin, from_far,
    load_sem, own_sem,
    z_send, z_recv, x_send, x_recv, half_send, half_recv,
    cot_send, cot_recv, step_send, step_recv, out_sem, turn,
):
    width = tok.shape[1]
    scale = width ** (-0.5)
    shard = tokens.shape[1]
    units = w_gate.shape[2]
    chunk = LINE * shard
    tall = 256
    blocks = width // tall

    g = lax.axis_index("grp")
    d = lax.axis_index("dp")
    z, x = d // LINE, d % LINE
    core = g % 2
    even = core == 0
    odd = core == 1
    twin = g + 1 - 2 * core
    far = (g - 1 + 2 * core + groups) % groups
    x_left, x_right, x_opp = (x + 3) % LINE, (x + 1) % LINE, (x + 2) % LINE

    def row_of(k):
        flip = z // 2
        low = z + flip * (3 - 2 * z)
        near = (1 - k // 2) * ((low + k) % 2) + (k // 2) * k
        return near + flip * (3 - 2 * near)

    barrier = pltpu.get_barrier_semaphore()

    def greet(i, carry):
        peer = (d + i) % 16
        pl.semaphore_signal(barrier, inc=1, device_id=(g, peer), device_id_type=MESH)
        return carry

    lax.fori_loop(1, 16, greet, 0)
    pl.semaphore_signal(barrier, inc=1, device_id=(twin, d), device_id_type=MESH)
    pl.semaphore_signal(barrier, inc=1, device_id=(far, d), device_id_type=MESH)

    def shard_at(row, col):
        return pl.ds(pl.multiple_of((row * LINE + col) * shard, shard), shard)

    loads = [
        pltpu.make_async_copy(tokens.at[0], tok.at[shard_at(z, x)], own_sem),
        pltpu.make_async_copy(w_gate.at[0], wts.at[:, pl.ds(0, units)], load_sem.at[0]),
        pltpu.make_async_copy(w_up.at[0], wts.at[:, pl.ds(units, units)], load_sem.at[1]),
        pltpu.make_async_copy(
            hidden_grad.at[0, :, pl.ds(pl.multiple_of(d * units, 128), units)],
            cot.at[shard_at(z, x)],
            load_sem.at[2],
        ),
    ]
    for load in loads:
        load.start()
    def meet():
        loads[0].wait()
        pl.semaphore_wait(barrier, 17)

    meet()

    part_rows = shard // PIECES

    def piece_at(row, col, p):
        return pl.ds(pl.multiple_of((row * LINE + col) * shard + p * part_rows, part_rows), part_rows)

    def z_copy(row, p, way, to):
        return pltpu.make_async_remote_copy(
            src_ref=tok.at[piece_at(row, x, p)],
            dst_ref=tok.at[piece_at(row, x, p)],
            send_sem=z_send.at[way, row, p],
            recv_sem=z_recv.at[row, p],
            device_id=(g, to * LINE + x),
            device_id_type=MESH,
        )

    def x_copy(row, col, p, way):
        to = x_right if way == 0 else x_left
        return pltpu.make_async_remote_copy(
            src_ref=tok.at[piece_at(row, col, p)],
            dst_ref=tok.at[piece_at(row, col, p)],
            send_sem=x_send.at[way, row, p],
            recv_sem=x_recv.at[way, row, p],
            device_id=(g, z * LINE + to),
            device_id_type=MESH,
        )

    def far_copy(row, col, way):
        to = x_right if way == 0 else x_left
        return pltpu.make_async_remote_copy(
            src_ref=tok.at[piece_at(row, col, way)],
            dst_ref=tok.at[piece_at(row, col, way)],
            send_sem=half_send.at[way, row],
            recv_sem=half_recv.at[way, row],
            device_id=(g, z * LINE + to),
            device_id_type=MESH,
        )

    def send_z(row, p):
        @pl.when((z < LINE - 1) & (row <= z))
        def _():
            z_copy(row, p, 0, z + 1).start()

        @pl.when((z > 0) & (row >= z))
        def _():
            z_copy(row, p, 1, z - 1).start()

    def take_z(row, p):
        z_copy(row, p, 0, z).wait_recv()
        send_z(row, p)

    def send_x(row, p):
        x_copy(row, x, p, 0).start()
        x_copy(row, x, p, 1).start()

    def relay_x(row):
        x_copy(row, x_left, 0, 0).wait_recv()
        far_copy(row, x_left, 0).start()
        x_copy(row, x_right, 1, 1).wait_recv()
        far_copy(row, x_right, 1).start()

    def cot_copy(peer):
        return pltpu.make_async_remote_copy(
            src_ref=hidden_grad.at[0, :, pl.ds(pl.multiple_of(peer * units, 128), units)],
            dst_ref=cot.at[shard_at(z, x)],
            send_sem=cot_send.at[peer],
            recv_sem=cot_recv.at[d],
            device_id=(g, peer),
            device_id_type=MESH,
        )

    def exchange(row):
        def one(i, carry):
            cot_copy(row * LINE + (x + 4 - i) % LINE).start()
            return carry

        lax.fori_loop(1, LINE, one, 0)

        @pl.when(row != z)
        def _():
            cot_copy(row * LINE + x).start()

    def exchange_inner():
        exchange(z)
        for row in range(1, LINE - 1):
            @pl.when(row != z)
            def _():
                exchange(row)

    def exchange_outer():
        for row in (0, LINE - 1):
            @pl.when(row != z)
            def _():
                exchange(row)

    def take_cot(source):
        pltpu.make_async_remote_copy(
            src_ref=cot.at[pl.ds(pl.multiple_of(source * shard, shard), shard)],
            dst_ref=cot.at[pl.ds(pl.multiple_of(source * shard, shard), shard)],
            send_sem=cot_send.at[0],
            recv_sem=cot_recv.at[source],
            device_id=(g, source),
            device_id_type=MESH,
        ).wait_recv()

    def gating(row):
        for col in (x_left, x_right, x_opp):
            take_cot(row * LINE + col)

        @pl.when(row != z)
        def _():
            take_cot(row * LINE + x)

        def part(m, carry):
            at = pl.ds(pl.multiple_of(row * chunk + m * tall, tall), tall)
            acc[...] = jnp.dot(tok[at, :], wts[...], preferred_element_type=jnp.float32)
            gate = acc[:, :units] * scale
            up = acc[:, units:] * scale
            sigma = jax.nn.sigmoid(gate)
            upstream = cot[at, :].astype(jnp.float32)
            rows[at, :units] = (upstream * up * sigma * (1.0 + gate * (1.0 - sigma))).astype(jnp.bfloat16)
            rows[at, units:] = (upstream * gate * sigma).astype(jnp.bfloat16)
            return carry

        lax.fori_loop(0, chunk // tall, part, 0)

    def gradient(b):
        to = pl.ds(pl.multiple_of(b * tall, tall), tall)
        return lax.dot_general(
            tok[:, to], rows[...], (((0,), (0,)), ((), ())), preferred_element_type=jnp.float32
        )

    def finish_row(row):
        x_copy(row, x_left, 1, 0).wait_recv()
        x_copy(row, x_right, 0, 1).wait_recv()
        far_copy(row, x_opp, 0).wait_recv()
        far_copy(row, x_opp, 1).wait_recv()
        gating(row)

    def my_turn(i):
        pl.semaphore_signal(turn.at[i], inc=1, device_id=(twin, d), device_id_type=MESH)

    def wait_turn(i):
        pl.semaphore_wait(turn.at[i], 1)

    @pl.when(odd)
    def _():
        if OUTER_ODD == 0:
            exchange_outer()
        if TURN_Z >= 0:
            wait_turn(0)

    for p in range(PIECES):
        send_z(z, p)

    @pl.when(even)
    def _():
        for p in range(PIECES):
            send_x(z, p)

    @pl.when(even)
    def _():
        if TURN_Z == 0:
            my_turn(0)

    if INNER_AT == 0:
        exchange_inner()

    for k in range(1, LINE):
        row = row_of(k)
        for p in range(PIECES):
            take_z(row, p)

            @pl.when(even)
            def _():
                send_x(row, p)

        @pl.when(even)
        def _():
            if k == TURN_Z:
                my_turn(0)
            relay_x(row_of(k - 1))

        if k == INNER_AT:
            exchange_inner()
        if k == OUTER_AT and k == OUTER_ODD:
            exchange_outer()
        elif k == OUTER_AT:
            pl.when(even)(exchange_outer)
        elif k == OUTER_ODD:
            pl.when(odd)(exchange_outer)

    for load in loads[1:]:
        load.wait()

    @pl.when(odd)
    def _():
        wait_turn(1)
        for k in range(LINE):
            for p in range(PIECES):
                send_x(row_of(k), p)
        for k in range(LINE - 1):
            relay_x(row_of(k))

    def all_rows(k, carry):
        finish_row(row_of(k))
        return carry

    lax.fori_loop(0, EARLY_ROWS, all_rows, 0)
    relay_x(row_of(LINE - 1))

    @pl.when(even)
    def _():
        my_turn(1)

    lax.fori_loop(EARLY_ROWS, LINE, all_rows, 0)

    def step_copy(b, way):
        to = pl.ds(pl.multiple_of(b * tall, tall), tall)
        return pltpu.make_async_remote_copy(
            src_ref=step.at[to],
            dst_ref=(from_twin if way == 0 else from_far).at[to],
            send_sem=step_send.at[way, b],
            recv_sem=step_recv.at[way, b],
            device_id=((twin if way == 0 else far), d),
            device_id_type=MESH,
        )

    def send_step(b):
        step_copy(b, 1).start()
        step_copy(b, 0).start()

    def final(b, carry):
        to = pl.ds(pl.multiple_of(b * tall, tall), tall)
        moved = wts[to, :].astype(jnp.float32) - 0.5 * (gradient(b) * scale)
        step[to, :] = moved.astype(jnp.bfloat16)

        @pl.when(b > 0)
        def _():
            send_step(b - 1)

        return carry

    lax.fori_loop(0, blocks, final, 0)
    send_step(blocks - 1)

    def out_copies(b):
        to = pl.ds(pl.multiple_of(b * tall, tall), tall)
        return (pltpu.make_async_copy(from_far.at[to], out.at[0, to], out_sem.at[b]),)

    def mix(b, carry):
        to = pl.ds(pl.multiple_of(b * tall, tall), tall)
        step_copy(b, 0).wait_recv()
        step_copy(b, 1).wait_recv()
        mixed = 0.5 * step[to, :].astype(jnp.float32) + 0.25 * (
            from_twin[to, :].astype(jnp.float32) + from_far[to, :].astype(jnp.float32)
        )
        from_far[to, :] = mixed.astype(jnp.bfloat16)
        for copy in out_copies(b):
            copy.start()
        return carry

    lax.fori_loop(0, blocks, mix, 0)

    def sent_rows(k, carry):
        row = row_of(k)

        for p in range(PIECES):
            @pl.when((z < LINE - 1) & (row <= z))
            def _():
                z_copy(row, p, 0, z + 1).wait_send()

            @pl.when((z > 0) & (row >= z))
            def _():
                z_copy(row, p, 1, z - 1).wait_send()

            x_copy(row, x, p, 0).wait_send()
            x_copy(row, x, p, 1).wait_send()

        far_copy(row, x_left, 0).wait_send()
        far_copy(row, x_right, 1).wait_send()
        return carry

    lax.fori_loop(0, LINE, sent_rows, 0)

    def sent_cot(i, carry):
        cot_copy((d + i) % 16).wait_send()
        return carry

    lax.fori_loop(1, 16, sent_cot, 0)

    def sent_blocks(b, carry):
        step_copy(b, 0).wait_send()
        step_copy(b, 1).wait_send()
        for copy in out_copies(b):
            copy.wait()
        return carry

    lax.fori_loop(0, blocks, sent_blocks, 0)


def solution(mesh):
    groups = mesh.shape["grp"]

    def local(tokens, hidden_grad, w_gate, w_up):
        shard, width = tokens.shape[1:]
        units = w_gate.shape[2]
        count = shard * mesh.shape["dp"]
        tall = 256
        blocks = width // tall
        dma = pltpu.SemaphoreType.DMA
        wide = 2 * units
        mixed = pl.pallas_call(
            functools.partial(kernel, groups),
            out_shape=jax.ShapeDtypeStruct((1, width, wide), jnp.bfloat16),
            in_specs=[pl.BlockSpec(memory_space=pl.ANY)] * 4,
            out_specs=pl.BlockSpec(memory_space=pl.ANY),
            scratch_shapes=[
                pltpu.VMEM((count, width), jnp.bfloat16),
                pltpu.VMEM((count, units), jnp.bfloat16),
                pltpu.VMEM((width, wide), jnp.bfloat16),
                pltpu.VMEM((count, wide), jnp.bfloat16),
                pltpu.VMEM((tall, wide), jnp.float32),
                pltpu.VMEM((width, wide), jnp.bfloat16),
                pltpu.VMEM((width, wide), jnp.bfloat16),
                pltpu.VMEM((width, wide), jnp.bfloat16),
                dma((3,)),
                dma(()),
                dma((2, LINE, PIECES)),
                dma((LINE, PIECES)),
                dma((2, LINE, PIECES)),
                dma((2, LINE, PIECES)),
                dma((2, LINE)),
                dma((2, LINE)),
                dma((16,)),
                dma((16,)),
                dma((2, blocks)),
                dma((2, blocks)),
                dma((blocks,)),
                pltpu.SemaphoreType.REGULAR((2,)),
            ],
            compiler_params=pltpu.CompilerParams(
                collective_id=0, has_side_effects=True, vmem_limit_bytes=60 * 1024 * 1024
            ),
        )(tokens, hidden_grad, w_gate, w_up)
        return mixed[:, :, :units], mixed[:, :, units:]

    in_specs = (
        P("grp", "dp", None),
        P("grp", "dp", None),
        P("grp", None, "dp"),
        P("grp", None, "dp"),
    )
    out_specs = (P("grp", None, "dp"), P("grp", None, "dp"))
    return jax.shard_map(local, mesh=mesh, in_specs=in_specs, out_specs=out_specs, check_vma=False)
```

```python
import functools

import jax
import jax.numpy as jnp
from jax import lax
from jax.experimental import pallas as pl
from jax.experimental.pallas import tpu as pltpu
from jax.sharding import PartitionSpec as P

MESH = pl.DeviceIdType.MESH
LINE = 4
PIECES = 2
TURN_Z = 2
INNER_AT = 1
OUTER_AT = 2
EARLY_ROWS = 1
OUTER_ODD = 0


def kernel(
    groups, tokens, hidden_grad, w_gate, w_up, out,
    tok, cot, wts, rows, acc, step, from_twin, from_far,
    load_sem, own_sem,
    z_send, z_recv, x_send, x_recv, half_send, half_recv,
    cot_send, cot_recv, step_send, step_recv, out_sem, turn,
):
    width = tok.shape[1]
    scale = width ** (-0.5)
    shard = tokens.shape[1]
    units = w_gate.shape[2]
    chunk = LINE * shard
    tall = 256
    blocks = width // tall

    g = lax.axis_index("grp")
    d = lax.axis_index("dp")
    z, x = d // LINE, d % LINE
    core = g % 2
    even = core == 0
    odd = core == 1
    twin = g + 1 - 2 * core
    far = (g - 1 + 2 * core + groups) % groups
    x_left, x_right, x_opp = (x + 3) % LINE, (x + 1) % LINE, (x + 2) % LINE

    def row_of(k):
        flip = z // 2
        low = z + flip * (3 - 2 * z)
        near = (1 - k // 2) * ((low + k) % 2) + (k // 2) * k
        return near + flip * (3 - 2 * near)

    barrier = pltpu.get_barrier_semaphore()

    def greet(i, carry):
        peer = (d + i) % 16
        pl.semaphore_signal(barrier, inc=1, device_id=(g, peer), device_id_type=MESH)
        return carry

    lax.fori_loop(1, 16, greet, 0)
    pl.semaphore_signal(barrier, inc=1, device_id=(twin, d), device_id_type=MESH)
    pl.semaphore_signal(barrier, inc=1, device_id=(far, d), device_id_type=MESH)

    def shard_at(row, col):
        return pl.ds(pl.multiple_of((row * LINE + col) * shard, shard), shard)

    loads = [
        pltpu.make_async_copy(tokens.at[0], tok.at[shard_at(z, x)], own_sem),
        pltpu.make_async_copy(w_gate.at[0], wts.at[:, pl.ds(0, units)], load_sem.at[0]),
        pltpu.make_async_copy(w_up.at[0], wts.at[:, pl.ds(units, units)], load_sem.at[1]),
        pltpu.make_async_copy(
            hidden_grad.at[0, :, pl.ds(pl.multiple_of(d * units, 128), units)],
            cot.at[shard_at(z, x)],
            load_sem.at[2],
        ),
    ]
    for load in loads:
        load.start()
    def meet():
        loads[0].wait()
        pl.semaphore_wait(barrier, 17)

    meet()

    part_rows = shard // PIECES

    def piece_at(row, col, p):
        return pl.ds(pl.multiple_of((row * LINE + col) * shard + p * part_rows, part_rows), part_rows)

    def z_copy(row, p, way, to):
        return pltpu.make_async_remote_copy(
            src_ref=tok.at[piece_at(row, x, p)],
            dst_ref=tok.at[piece_at(row, x, p)],
            send_sem=z_send.at[way, row, p],
            recv_sem=z_recv.at[row, p],
            device_id=(g, to * LINE + x),
            device_id_type=MESH,
        )

    def x_copy(row, col, p, way):
        to = x_right if way == 0 else x_left
        return pltpu.make_async_remote_copy(
            src_ref=tok.at[piece_at(row, col, p)],
            dst_ref=tok.at[piece_at(row, col, p)],
            send_sem=x_send.at[way, row, p],
            recv_sem=x_recv.at[way, row, p],
            device_id=(g, z * LINE + to),
            device_id_type=MESH,
        )

    def far_copy(row, col, way):
        to = x_right if way == 0 else x_left
        return pltpu.make_async_remote_copy(
            src_ref=tok.at[piece_at(row, col, way)],
            dst_ref=tok.at[piece_at(row, col, way)],
            send_sem=half_send.at[way, row],
            recv_sem=half_recv.at[way, row],
            device_id=(g, z * LINE + to),
            device_id_type=MESH,
        )

    def send_z(row, p):
        @pl.when((z < LINE - 1) & (row <= z))
        def _():
            z_copy(row, p, 0, z + 1).start()

        @pl.when((z > 0) & (row >= z))
        def _():
            z_copy(row, p, 1, z - 1).start()

    def take_z(row, p):
        z_copy(row, p, 0, z).wait_recv()
        send_z(row, p)

    def send_x(row, p):
        x_copy(row, x, p, 0).start()
        x_copy(row, x, p, 1).start()

    def relay_x(row):
        x_copy(row, x_left, 0, 0).wait_recv()
        far_copy(row, x_left, 0).start()
        x_copy(row, x_right, 1, 1).wait_recv()
        far_copy(row, x_right, 1).start()

    def cot_copy(peer):
        return pltpu.make_async_remote_copy(
            src_ref=hidden_grad.at[0, :, pl.ds(pl.multiple_of(peer * units, 128), units)],
            dst_ref=cot.at[shard_at(z, x)],
            send_sem=cot_send.at[peer],
            recv_sem=cot_recv.at[d],
            device_id=(g, peer),
            device_id_type=MESH,
        )

    def exchange(row):
        def one(i, carry):
            cot_copy(row * LINE + (x + 4 - i) % LINE).start()
            return carry

        lax.fori_loop(1, LINE, one, 0)

        @pl.when(row != z)
        def _():
            cot_copy(row * LINE + x).start()

    def exchange_inner():
        exchange(z)
        for row in range(1, LINE - 1):
            @pl.when(row != z)
            def _():
                exchange(row)

    def exchange_outer():
        for row in (0, LINE - 1):
            @pl.when(row != z)
            def _():
                exchange(row)

    def take_cot(source):
        pltpu.make_async_remote_copy(
            src_ref=cot.at[pl.ds(pl.multiple_of(source * shard, shard), shard)],
            dst_ref=cot.at[pl.ds(pl.multiple_of(source * shard, shard), shard)],
            send_sem=cot_send.at[0],
            recv_sem=cot_recv.at[source],
            device_id=(g, source),
            device_id_type=MESH,
        ).wait_recv()

    def gating(row):
        for col in (x_left, x_right, x_opp):
            take_cot(row * LINE + col)

        @pl.when(row != z)
        def _():
            take_cot(row * LINE + x)

        def part(m, carry):
            at = pl.ds(pl.multiple_of(row * chunk + m * tall, tall), tall)
            acc[...] = jnp.dot(tok[at, :], wts[...], preferred_element_type=jnp.float32)
            gate = acc[:, :units] * scale
            up = acc[:, units:] * scale
            sigma = jax.nn.sigmoid(gate)
            upstream = cot[at, :].astype(jnp.float32)
            rows[at, :units] = (upstream * up * sigma * (1.0 + gate * (1.0 - sigma))).astype(jnp.bfloat16)
            rows[at, units:] = (upstream * gate * sigma).astype(jnp.bfloat16)
            return carry

        lax.fori_loop(0, chunk // tall, part, 0)

    def gradient(b):
        to = pl.ds(pl.multiple_of(b * tall, tall), tall)
        return lax.dot_general(
            tok[:, to], rows[...], (((0,), (0,)), ((), ())), preferred_element_type=jnp.float32
        )

    def finish_row(row):
        x_copy(row, x_left, 1, 0).wait_recv()
        x_copy(row, x_right, 0, 1).wait_recv()
        far_copy(row, x_opp, 0).wait_recv()
        far_copy(row, x_opp, 1).wait_recv()
        gating(row)

    def my_turn(i):
        pl.semaphore_signal(turn.at[i], inc=1, device_id=(twin, d), device_id_type=MESH)

    def wait_turn(i):
        pl.semaphore_wait(turn.at[i], 1)

    @pl.when(odd)
    def _():
        if OUTER_ODD == 0:
            exchange_outer()
        if TURN_Z >= 0:
            wait_turn(0)

    for p in range(PIECES):
        send_z(z, p)

    @pl.when(even)
    def _():
        for p in range(PIECES):
            send_x(z, p)

    @pl.when(even)
    def _():
        if TURN_Z == 0:
            my_turn(0)

    if INNER_AT == 0:
        exchange_inner()

    for k in range(1, LINE):
        row = row_of(k)
        for p in range(PIECES):
            take_z(row, p)

            @pl.when(even)
            def _():
                send_x(row, p)

        @pl.when(even)
        def _():
            if k == TURN_Z:
                my_turn(0)
            relay_x(row_of(k - 1))

        if k == INNER_AT:
            exchange_inner()
        if k == OUTER_AT and k == OUTER_ODD:
            exchange_outer()
        elif k == OUTER_AT:
            pl.when(even)(exchange_outer)
        elif k == OUTER_ODD:
            pl.when(odd)(exchange_outer)

    for load in loads[1:]:
        load.wait()

    @pl.when(odd)
    def _():
        wait_turn(1)
        for k in range(LINE):
            for p in range(PIECES):
                send_x(row_of(k), p)
        for k in range(LINE - 1):
            relay_x(row_of(k))

    def all_rows(k, carry):
        finish_row(row_of(k))
        return carry

    lax.fori_loop(0, EARLY_ROWS, all_rows, 0)
    relay_x(row_of(LINE - 1))

    @pl.when(even)
    def _():
        my_turn(1)

    lax.fori_loop(EARLY_ROWS, LINE, all_rows, 0)

    def step_copy(b, way):
        to = pl.ds(pl.multiple_of(b * tall, tall), tall)
        return pltpu.make_async_remote_copy(
            src_ref=step.at[to],
            dst_ref=(from_twin if way == 0 else from_far).at[to],
            send_sem=step_send.at[way, b],
            recv_sem=step_recv.at[way, b],
            device_id=((twin if way == 0 else far), d),
            device_id_type=MESH,
        )

    def send_step(b):
        step_copy(b, 1).start()
        step_copy(b, 0).start()

    def final(b, carry):
        to = pl.ds(pl.multiple_of(b * tall, tall), tall)
        moved = wts[to, :].astype(jnp.float32) - 0.5 * (gradient(b) * scale)
        step[to, :] = moved.astype(jnp.bfloat16)

        @pl.when(b > 0)
        def _():
            send_step(b - 1)

        return carry

    lax.fori_loop(0, blocks, final, 0)
    send_step(blocks - 1)

    def out_copies(b):
        to = pl.ds(pl.multiple_of(b * tall, tall), tall)
        return (pltpu.make_async_copy(from_far.at[to], out.at[0, to], out_sem.at[b]),)

    def mix(b, carry):
        to = pl.ds(pl.multiple_of(b * tall, tall), tall)
        step_copy(b, 0).wait_recv()
        step_copy(b, 1).wait_recv()
        mixed = 0.5 * step[to, :].astype(jnp.float32) + 0.25 * (
            from_twin[to, :].astype(jnp.float32) + from_far[to, :].astype(jnp.float32)
        )
        from_far[to, :] = mixed.astype(jnp.bfloat16)
        for copy in out_copies(b):
            copy.start()
        return carry

    lax.fori_loop(0, blocks, mix, 0)

    def sent_rows(k, carry):
        row = row_of(k)

        for p in range(PIECES):
            @pl.when((z < LINE - 1) & (row <= z))
            def _():
                z_copy(row, p, 0, z + 1).wait_send()

            @pl.when((z > 0) & (row >= z))
            def _():
                z_copy(row, p, 1, z - 1).wait_send()

            x_copy(row, x, p, 0).wait_send()
            x_copy(row, x, p, 1).wait_send()

        far_copy(row, x_left, 0).wait_send()
        far_copy(row, x_right, 1).wait_send()
        return carry

    lax.fori_loop(0, LINE, sent_rows, 0)

    def sent_cot(i, carry):
        cot_copy((d + i) % 16).wait_send()
        return carry

    lax.fori_loop(1, 16, sent_cot, 0)

    def sent_blocks(b, carry):
        step_copy(b, 0).wait_send()
        step_copy(b, 1).wait_send()
        for copy in out_copies(b):
            copy.wait()
        return carry

    lax.fori_loop(0, blocks, sent_blocks, 0)


def split(mixed, out_gate, out_up, held, in_sem, out_sem):
    units = out_gate.shape[2]
    blocks = in_sem.shape[0]
    tall = held.shape[0] // blocks

    def take(b):
        at = pl.ds(b * tall, tall)
        return pltpu.make_async_copy(mixed.at[0, at], held.at[at], in_sem.at[b])

    def give(b):
        at = pl.ds(b * tall, tall)
        return (
            pltpu.make_async_copy(held.at[at, pl.ds(0, units)], out_gate.at[0, at], out_sem.at[0, b]),
            pltpu.make_async_copy(held.at[at, pl.ds(units, units)], out_up.at[0, at], out_sem.at[1, b]),
        )

    for b in range(blocks):
        take(b).start()
    for b in range(blocks):
        take(b).wait()
        for copy in give(b):
            copy.start()
    for b in range(blocks):
        for copy in give(b):
            copy.wait()


def solution(mesh):
    groups = mesh.shape["grp"]

    def local(tokens, hidden_grad, w_gate, w_up):
        shard, width = tokens.shape[1:]
        units = w_gate.shape[2]
        count = shard * mesh.shape["dp"]
        tall = 256
        blocks = width // tall
        dma = pltpu.SemaphoreType.DMA
        wide = 2 * units
        mixed = pl.pallas_call(
            functools.partial(kernel, groups),
            out_shape=jax.ShapeDtypeStruct((1, width, wide), jnp.bfloat16),
            in_specs=[pl.BlockSpec(memory_space=pl.ANY)] * 4,
            out_specs=pl.BlockSpec(memory_space=pl.ANY),
            scratch_shapes=[
                pltpu.VMEM((count, width), jnp.bfloat16),
                pltpu.VMEM((count, units), jnp.bfloat16),
                pltpu.VMEM((width, wide), jnp.bfloat16),
                pltpu.VMEM((count, wide), jnp.bfloat16),
                pltpu.VMEM((tall, wide), jnp.float32),
                pltpu.VMEM((width, wide), jnp.bfloat16),
                pltpu.VMEM((width, wide), jnp.bfloat16),
                pltpu.VMEM((width, wide), jnp.bfloat16),
                dma((3,)),
                dma(()),
                dma((2, LINE, PIECES)),
                dma((LINE, PIECES)),
                dma((2, LINE, PIECES)),
                dma((2, LINE, PIECES)),
                dma((2, LINE)),
                dma((2, LINE)),
                dma((16,)),
                dma((16,)),
                dma((2, blocks)),
                dma((2, blocks)),
                dma((blocks,)),
                pltpu.SemaphoreType.REGULAR((2,)),
            ],
            compiler_params=pltpu.CompilerParams(
                collective_id=0, has_side_effects=True, vmem_limit_bytes=60 * 1024 * 1024
            ),
        )(tokens, hidden_grad, w_gate, w_up)
        out = jax.ShapeDtypeStruct(w_gate.shape, jnp.bfloat16)
        return pl.pallas_call(
            split,
            out_shape=(out, out),
            in_specs=[pl.BlockSpec(memory_space=pl.ANY)],
            out_specs=(pl.BlockSpec(memory_space=pl.ANY),) * 2,
            scratch_shapes=[pltpu.VMEM((width, wide), jnp.bfloat16), dma((blocks,)), dma((2, blocks))],
            compiler_params=pltpu.CompilerParams(vmem_limit_bytes=60 * 1024 * 1024),
        )(mixed)

    in_specs = (
        P("grp", "dp", None),
        P("grp", "dp", None),
        P("grp", None, "dp"),
        P("grp", None, "dp"),
    )
    out_specs = (P("grp", None, "dp"), P("grp", None, "dp"))
    return jax.shard_map(local, mesh=mesh, in_specs=in_specs, out_specs=out_specs, check_vma=False)
```

```python
import functools

import jax
import jax.numpy as jnp
from jax import lax
from jax.experimental import pallas as pl
from jax.experimental.pallas import tpu as pltpu
from jax.sharding import PartitionSpec as P

MESH = pl.DeviceIdType.MESH
LINE = 4
PIECES = 4
TURN_Z = 2
INNER_AT = 1
OUTER_AT = 2
EARLY_ROWS = 1
OUTER_ODD = 0


def kernel(
    groups, tokens, hidden_grad, w_gate, w_up, out,
    tok, cot, held, wts, rows, acc, step, from_twin, from_far,
    load_sem, own_sem,
    z_send, z_recv, x_send, x_recv, half_send, half_recv,
    cot_send, cot_recv, step_send, step_recv, out_sem, turn,
):
    width = tok.shape[1]
    scale = width ** (-0.5)
    shard = tokens.shape[1]
    units = w_gate.shape[2]
    chunk = LINE * shard
    tall = 256
    blocks = width // tall

    g = lax.axis_index("grp")
    d = lax.axis_index("dp")
    z, x = d // LINE, d % LINE
    core = g % 2
    even = core == 0
    odd = core == 1
    twin = g + 1 - 2 * core
    far = (g - 1 + 2 * core + groups) % groups
    x_left, x_right, x_opp = (x + 3) % LINE, (x + 1) % LINE, (x + 2) % LINE

    def row_of(k):
        flip = z // 2
        low = z + flip * (3 - 2 * z)
        near = (1 - k // 2) * ((low + k) % 2) + (k // 2) * k
        return near + flip * (3 - 2 * near)

    barrier = pltpu.get_barrier_semaphore()

    def greet(i, carry):
        peer = (d + i) % 16
        pl.semaphore_signal(barrier, inc=1, device_id=(g, peer), device_id_type=MESH)
        return carry

    lax.fori_loop(1, 16, greet, 0)
    pl.semaphore_signal(barrier, inc=1, device_id=(twin, d), device_id_type=MESH)
    pl.semaphore_signal(barrier, inc=1, device_id=(far, d), device_id_type=MESH)

    def shard_at(row, col):
        return pl.ds(pl.multiple_of((row * LINE + col) * shard, shard), shard)

    loads = [
        pltpu.make_async_copy(tokens.at[0], tok.at[shard_at(z, x)], own_sem),
        pltpu.make_async_copy(w_gate.at[0], wts.at[:, pl.ds(0, units)], load_sem.at[0]),
        pltpu.make_async_copy(w_up.at[0], wts.at[:, pl.ds(units, units)], load_sem.at[1]),
        pltpu.make_async_copy(
            hidden_grad.at[0, :, pl.ds(pl.multiple_of(d * units, 128), units)],
            cot.at[shard_at(z, x)],
            load_sem.at[2],
        ),
        pltpu.make_async_copy(hidden_grad.at[0], held, load_sem.at[3]),
    ]
    for load in (loads[0], loads[4], *loads[1:4]):
        load.start()
    def meet():
        loads[0].wait()
        loads[4].wait()
        pl.semaphore_wait(barrier, 17)

    meet()

    part_rows = shard // PIECES

    def piece_at(row, col, p):
        return pl.ds(pl.multiple_of((row * LINE + col) * shard + p * part_rows, part_rows), part_rows)

    def z_copy(row, p, way, to):
        return pltpu.make_async_remote_copy(
            src_ref=tok.at[piece_at(row, x, p)],
            dst_ref=tok.at[piece_at(row, x, p)],
            send_sem=z_send.at[way, row, p],
            recv_sem=z_recv.at[row, p],
            device_id=(g, to * LINE + x),
            device_id_type=MESH,
        )

    def x_copy(row, col, p, way):
        to = x_right if way == 0 else x_left
        return pltpu.make_async_remote_copy(
            src_ref=tok.at[piece_at(row, col, p)],
            dst_ref=tok.at[piece_at(row, col, p)],
            send_sem=x_send.at[way, row, p],
            recv_sem=x_recv.at[way, row, p],
            device_id=(g, z * LINE + to),
            device_id_type=MESH,
        )

    def far_copy(row, col, p, way):
        to = x_right if way == 0 else x_left
        return pltpu.make_async_remote_copy(
            src_ref=tok.at[piece_at(row, col, p)],
            dst_ref=tok.at[piece_at(row, col, p)],
            send_sem=half_send.at[way, row, p],
            recv_sem=half_recv.at[way, row, p],
            device_id=(g, z * LINE + to),
            device_id_type=MESH,
        )

    def send_z(row, p):
        @pl.when((z < LINE - 1) & (row <= z))
        def _():
            z_copy(row, p, 0, z + 1).start()

        @pl.when((z > 0) & (row >= z))
        def _():
            z_copy(row, p, 1, z - 1).start()

    def take_z(row, p):
        z_copy(row, p, 0, z).wait_recv()
        send_z(row, p)

    def send_x(row, p):
        x_copy(row, x, p, 0).start()
        x_copy(row, x, p, 1).start()

    near = range(PIECES // 2)
    back = range(PIECES // 2, PIECES)

    def relay_x(row):
        for p, q in zip(near, back):
            x_copy(row, x_left, p, 0).wait_recv()
            far_copy(row, x_left, p, 0).start()
            x_copy(row, x_right, q, 1).wait_recv()
            far_copy(row, x_right, q, 1).start()

    def cot_copy(peer):
        return pltpu.make_async_remote_copy(
            src_ref=held.at[:, pl.ds(pl.multiple_of(peer * units, 128), units)],
            dst_ref=cot.at[shard_at(z, x)],
            send_sem=cot_send.at[peer],
            recv_sem=cot_recv.at[d],
            device_id=(g, peer),
            device_id_type=MESH,
        )

    def exchange(row):
        def one(i, carry):
            cot_copy(row * LINE + (x + 4 - i) % LINE).start()
            return carry

        lax.fori_loop(1, LINE, one, 0)

        @pl.when(row != z)
        def _():
            cot_copy(row * LINE + x).start()

    def exchange_inner():
        exchange(z)
        for row in range(1, LINE - 1):
            @pl.when(row != z)
            def _():
                exchange(row)

    def exchange_outer():
        for row in (0, LINE - 1):
            @pl.when(row != z)
            def _():
                exchange(row)

    def take_cot(source):
        pltpu.make_async_remote_copy(
            src_ref=cot.at[pl.ds(pl.multiple_of(source * shard, shard), shard)],
            dst_ref=cot.at[pl.ds(pl.multiple_of(source * shard, shard), shard)],
            send_sem=cot_send.at[0],
            recv_sem=cot_recv.at[source],
            device_id=(g, source),
            device_id_type=MESH,
        ).wait_recv()

    def gating(row):
        for col in (x_left, x_right, x_opp):
            take_cot(row * LINE + col)

        @pl.when(row != z)
        def _():
            take_cot(row * LINE + x)

        def part(m, carry):
            at = pl.ds(pl.multiple_of(row * chunk + m * tall, tall), tall)
            acc[...] = jnp.dot(tok[at, :], wts[...], preferred_element_type=jnp.float32)
            gate = acc[:, :units] * scale
            up = acc[:, units:] * scale
            sigma = jax.nn.sigmoid(gate)
            upstream = cot[at, :].astype(jnp.float32)
            rows[at, :units] = (upstream * up * sigma * (1.0 + gate * (1.0 - sigma))).astype(jnp.bfloat16)
            rows[at, units:] = (upstream * gate * sigma).astype(jnp.bfloat16)
            return carry

        lax.fori_loop(0, chunk // tall, part, 0)

    def gradient(b):
        to = pl.ds(pl.multiple_of(b * tall, tall), tall)
        return lax.dot_general(
            tok[:, to], rows[...], (((0,), (0,)), ((), ())), preferred_element_type=jnp.float32
        )

    def finish_row(row):
        for p, q in zip(near, back):
            x_copy(row, x_left, q, 0).wait_recv()
            x_copy(row, x_right, p, 1).wait_recv()
            far_copy(row, x_opp, p, 0).wait_recv()
            far_copy(row, x_opp, q, 1).wait_recv()
        gating(row)

    def my_turn(i):
        pl.semaphore_signal(turn.at[i], inc=1, device_id=(twin, d), device_id_type=MESH)

    def wait_turn(i):
        pl.semaphore_wait(turn.at[i], 1)

    @pl.when(odd)
    def _():
        if OUTER_ODD == 0:
            exchange_outer()
        if TURN_Z >= 0:
            wait_turn(0)

    for p in range(PIECES):
        send_z(z, p)

    @pl.when(even)
    def _():
        for p in range(PIECES):
            send_x(z, p)

    @pl.when(even)
    def _():
        if TURN_Z == 0:
            my_turn(0)

    if INNER_AT == 0:
        exchange_inner()

    for k in range(1, LINE):
        row = row_of(k)
        for p in range(PIECES):
            take_z(row, p)

            @pl.when(even)
            def _():
                send_x(row, p)

        @pl.when(even)
        def _():
            if k == TURN_Z:
                my_turn(0)
            relay_x(row_of(k - 1))

        if k == INNER_AT:
            exchange_inner()
        if k == OUTER_AT and k == OUTER_ODD:
            exchange_outer()
        elif k == OUTER_AT:
            pl.when(even)(exchange_outer)
        elif k == OUTER_ODD:
            pl.when(odd)(exchange_outer)

    for load in loads[1:4]:
        load.wait()

    @pl.when(odd)
    def _():
        wait_turn(1)
        for k in range(LINE):
            for p in range(PIECES):
                send_x(row_of(k), p)
        for k in range(LINE - 1):
            relay_x(row_of(k))

    def all_rows(k, carry):
        finish_row(row_of(k))
        return carry

    lax.fori_loop(0, EARLY_ROWS, all_rows, 0)
    relay_x(row_of(LINE - 1))

    @pl.when(even)
    def _():
        my_turn(1)

    lax.fori_loop(EARLY_ROWS, LINE, all_rows, 0)

    def step_copy(b, way):
        to = pl.ds(pl.multiple_of(b * tall, tall), tall)
        return pltpu.make_async_remote_copy(
            src_ref=step.at[to],
            dst_ref=(from_twin if way == 0 else from_far).at[to],
            send_sem=step_send.at[way, b],
            recv_sem=step_recv.at[way, b],
            device_id=((twin if way == 0 else far), d),
            device_id_type=MESH,
        )

    def send_step(b):
        step_copy(b, 1).start()
        step_copy(b, 0).start()

    def final(b, carry):
        to = pl.ds(pl.multiple_of(b * tall, tall), tall)
        moved = wts[to, :].astype(jnp.float32) - 0.5 * (gradient(b) * scale)
        step[to, :] = moved.astype(jnp.bfloat16)

        @pl.when(b > 0)
        def _():
            send_step(b - 1)

        return carry

    lax.fori_loop(0, blocks, final, 0)
    send_step(blocks - 1)

    def sent_rows(k, carry):
        row = row_of(k)

        for p in range(PIECES):
            @pl.when((z < LINE - 1) & (row <= z))
            def _():
                z_copy(row, p, 0, z + 1).wait_send()

            @pl.when((z > 0) & (row >= z))
            def _():
                z_copy(row, p, 1, z - 1).wait_send()

            x_copy(row, x, p, 0).wait_send()
            x_copy(row, x, p, 1).wait_send()

        for p, q in zip(near, back):
            far_copy(row, x_left, p, 0).wait_send()
            far_copy(row, x_right, q, 1).wait_send()

        return carry

    lax.fori_loop(0, LINE, sent_rows, 0)

    def sent_cot(i, carry):
        cot_copy((d + i) % 16).wait_send()
        return carry

    lax.fori_loop(1, 16, sent_cot, 0)

    def out_copies(b):
        to = pl.ds(pl.multiple_of(b * tall, tall), tall)
        return (pltpu.make_async_copy(from_far.at[to], out.at[0, to], out_sem.at[b]),)

    def mix(b, carry):
        to = pl.ds(pl.multiple_of(b * tall, tall), tall)
        step_copy(b, 0).wait_recv()
        step_copy(b, 1).wait_recv()
        mixed = 0.5 * step[to, :].astype(jnp.float32) + 0.25 * (
            from_twin[to, :].astype(jnp.float32) + from_far[to, :].astype(jnp.float32)
        )
        from_far[to, :] = mixed.astype(jnp.bfloat16)

        @pl.when(b > 0)
        def _():
            for copy in out_copies(b - 1):
                copy.start()

        return carry

    lax.fori_loop(0, blocks, mix, 0)
    for copy in out_copies(blocks - 1):
        copy.start()

    def sent_blocks(b, carry):
        step_copy(b, 0).wait_send()
        step_copy(b, 1).wait_send()
        for copy in out_copies(b):
            copy.wait()
        return carry

    lax.fori_loop(0, blocks, sent_blocks, 0)


def split(mixed, out_gate, out_up, held, in_sem, out_sem):
    units = out_gate.shape[2]
    blocks = in_sem.shape[0]
    tall = held.shape[0] // blocks

    def take(b):
        at = pl.ds(b * tall, tall)
        return pltpu.make_async_copy(mixed.at[0, at], held.at[at], in_sem.at[b])

    def give(b):
        at = pl.ds(b * tall, tall)
        return (
            pltpu.make_async_copy(held.at[at, pl.ds(0, units)], out_gate.at[0, at], out_sem.at[0, b]),
            pltpu.make_async_copy(held.at[at, pl.ds(units, units)], out_up.at[0, at], out_sem.at[1, b]),
        )

    for b in range(blocks):
        take(b).start()
    for b in range(blocks):
        take(b).wait()
        for copy in give(b):
            copy.start()
    for b in range(blocks):
        for copy in give(b):
            copy.wait()


def solution(mesh):
    groups = mesh.shape["grp"]

    def local(tokens, hidden_grad, w_gate, w_up):
        shard, width = tokens.shape[1:]
        units = w_gate.shape[2]
        count = shard * mesh.shape["dp"]
        tall = 256
        blocks = width // tall
        dma = pltpu.SemaphoreType.DMA
        wide = 2 * units
        mixed = pl.pallas_call(
            functools.partial(kernel, groups),
            out_shape=jax.ShapeDtypeStruct((1, width, wide), jnp.bfloat16),
            in_specs=[pl.BlockSpec(memory_space=pl.ANY)] * 4,
            out_specs=pl.BlockSpec(memory_space=pl.ANY),
            scratch_shapes=[
                pltpu.VMEM((count, width), jnp.bfloat16),
                pltpu.VMEM((count, units), jnp.bfloat16),
                pltpu.VMEM(hidden_grad.shape[1:], jnp.bfloat16),
                pltpu.VMEM((width, wide), jnp.bfloat16),
                pltpu.VMEM((count, wide), jnp.bfloat16),
                pltpu.VMEM((tall, wide), jnp.float32),
                pltpu.VMEM((width, wide), jnp.bfloat16),
                pltpu.VMEM((width, wide), jnp.bfloat16),
                pltpu.VMEM((width, wide), jnp.bfloat16),
                dma((4,)),
                dma(()),
                dma((2, LINE, PIECES)),
                dma((LINE, PIECES)),
                dma((2, LINE, PIECES)),
                dma((2, LINE, PIECES)),
                dma((2, LINE, PIECES)),
                dma((2, LINE, PIECES)),
                dma((16,)),
                dma((16,)),
                dma((2, blocks)),
                dma((2, blocks)),
                dma((blocks,)),
                pltpu.SemaphoreType.REGULAR((2,)),
            ],
            compiler_params=pltpu.CompilerParams(
                collective_id=0, has_side_effects=True, vmem_limit_bytes=60 * 1024 * 1024
            ),
        )(tokens, hidden_grad, w_gate, w_up)
        out = jax.ShapeDtypeStruct(w_gate.shape, jnp.bfloat16)
        return pl.pallas_call(
            split,
            out_shape=(out, out),
            in_specs=[pl.BlockSpec(memory_space=pl.ANY)],
            out_specs=(pl.BlockSpec(memory_space=pl.ANY),) * 2,
            scratch_shapes=[pltpu.VMEM((width, wide), jnp.bfloat16), dma((4,)), dma((2, 4))],
            compiler_params=pltpu.CompilerParams(vmem_limit_bytes=60 * 1024 * 1024),
        )(mixed)

    in_specs = (
        P("grp", "dp", None),
        P("grp", "dp", None),
        P("grp", None, "dp"),
        P("grp", None, "dp"),
    )
    out_specs = (P("grp", None, "dp"), P("grp", None, "dp"))
    return jax.shard_map(local, mesh=mesh, in_specs=in_specs, out_specs=out_specs, check_vma=False)
```

```python
import functools

import jax
import jax.numpy as jnp
from jax import lax
from jax.experimental import pallas as pl
from jax.experimental.pallas import tpu as pltpu
from jax.sharding import PartitionSpec as P

MESH = pl.DeviceIdType.MESH
LINE = 4
PIECES = 4
TURN_Z = 2
INNER_AT = 1
OUTER_AT = 2
EARLY_ROWS = 1
OUTER_ODD = 0


def kernel(
    groups, tokens, hidden_grad, w_gate, w_up, out,
    tok, cot, held, wts, rows, acc, step, from_twin, from_far,
    load_sem, own_sem,
    z_send, z_recv, x_send, x_recv, half_send, half_recv,
    cot_send, cot_recv, step_send, step_recv, out_sem, turn,
):
    width = tok.shape[1]
    scale = width ** (-0.5)
    shard = tokens.shape[1]
    units = w_gate.shape[2]
    chunk = LINE * shard
    tall = 256
    blocks = width // tall

    g = lax.axis_index("grp")
    d = lax.axis_index("dp")
    z, x = d // LINE, d % LINE
    core = g % 2
    even = core == 0
    odd = core == 1
    twin = g + 1 - 2 * core
    far = (g - 1 + 2 * core + groups) % groups
    x_left, x_right, x_opp = (x + 3) % LINE, (x + 1) % LINE, (x + 2) % LINE

    def row_of(k):
        flip = z // 2
        low = z + flip * (3 - 2 * z)
        near = (1 - k // 2) * ((low + k) % 2) + (k // 2) * k
        return near + flip * (3 - 2 * near)

    barrier = pltpu.get_barrier_semaphore()

    def greet(group, peer):
        pl.semaphore_signal(barrier, inc=1, device_id=(group, peer), device_id_type=MESH)

    greet(far, d)
    for i in (8, 12, 4, 9, 11, 13, 7, 10, 6, 14, 5, 3, 15, 2, 1):
        greet(g, (d + i) % 16)
    greet(twin, d)

    def shard_at(row, col):
        return pl.ds(pl.multiple_of((row * LINE + col) * shard, shard), shard)

    loads = [
        pltpu.make_async_copy(tokens.at[0], tok.at[shard_at(z, x)], own_sem),
        pltpu.make_async_copy(w_gate.at[0], wts.at[:, pl.ds(0, units)], load_sem.at[0]),
        pltpu.make_async_copy(w_up.at[0], wts.at[:, pl.ds(units, units)], load_sem.at[1]),
        pltpu.make_async_copy(
            hidden_grad.at[0, :, pl.ds(pl.multiple_of(d * units, 128), units)],
            cot.at[shard_at(z, x)],
            load_sem.at[2],
        ),
        pltpu.make_async_copy(hidden_grad.at[0], held, load_sem.at[3]),
    ]
    for load in (loads[0], loads[4], *loads[1:4]):
        load.start()
    def meet():
        loads[0].wait()
        loads[4].wait()
        pl.semaphore_wait(barrier, 17)

    meet()

    part_rows = shard // PIECES

    def piece_at(row, col, p):
        return pl.ds(pl.multiple_of((row * LINE + col) * shard + p * part_rows, part_rows), part_rows)

    def z_copy(row, p, way, to):
        return pltpu.make_async_remote_copy(
            src_ref=tok.at[piece_at(row, x, p)],
            dst_ref=tok.at[piece_at(row, x, p)],
            send_sem=z_send.at[way, row, p],
            recv_sem=z_recv.at[row, p],
            device_id=(g, to * LINE + x),
            device_id_type=MESH,
        )

    def x_copy(row, col, p, way):
        to = x_right if way == 0 else x_left
        return pltpu.make_async_remote_copy(
            src_ref=tok.at[piece_at(row, col, p)],
            dst_ref=tok.at[piece_at(row, col, p)],
            send_sem=x_send.at[way, row, p],
            recv_sem=x_recv.at[way, row, p],
            device_id=(g, z * LINE + to),
            device_id_type=MESH,
        )

    def far_copy(row, col, p, way):
        to = x_right if way == 0 else x_left
        return pltpu.make_async_remote_copy(
            src_ref=tok.at[piece_at(row, col, p)],
            dst_ref=tok.at[piece_at(row, col, p)],
            send_sem=half_send.at[way, row, p],
            recv_sem=half_recv.at[way, row, p],
            device_id=(g, z * LINE + to),
            device_id_type=MESH,
        )

    def send_z(row, p):
        @pl.when((z < LINE - 1) & (row <= z))
        def _():
            z_copy(row, p, 0, z + 1).start()

        @pl.when((z > 0) & (row >= z))
        def _():
            z_copy(row, p, 1, z - 1).start()

    def take_z(row, p):
        z_copy(row, p, 0, z).wait_recv()
        send_z(row, p)

    def send_x(row, p):
        x_copy(row, x, p, 0).start()
        x_copy(row, x, p, 1).start()

    near = range(PIECES // 2)
    back = range(PIECES // 2, PIECES)

    def relay_x(row):
        for p, q in zip(near, back):
            x_copy(row, x_left, p, 0).wait_recv()
            far_copy(row, x_left, p, 0).start()
            x_copy(row, x_right, q, 1).wait_recv()
            far_copy(row, x_right, q, 1).start()

    def cot_copy(peer):
        return pltpu.make_async_remote_copy(
            src_ref=held.at[:, pl.ds(pl.multiple_of(peer * units, 128), units)],
            dst_ref=cot.at[shard_at(z, x)],
            send_sem=cot_send.at[peer],
            recv_sem=cot_recv.at[d],
            device_id=(g, peer),
            device_id_type=MESH,
        )

    def exchange(row):
        def one(i, carry):
            cot_copy(row * LINE + (x + 4 - i) % LINE).start()
            return carry

        lax.fori_loop(1, LINE, one, 0)

        @pl.when(row != z)
        def _():
            cot_copy(row * LINE + x).start()

    def exchange_inner():
        exchange(z)
        for row in range(1, LINE - 1):
            @pl.when(row != z)
            def _():
                exchange(row)

    def exchange_outer():
        for row in (0, LINE - 1):
            @pl.when(row != z)
            def _():
                exchange(row)

    def take_cot(source):
        pltpu.make_async_remote_copy(
            src_ref=cot.at[pl.ds(pl.multiple_of(source * shard, shard), shard)],
            dst_ref=cot.at[pl.ds(pl.multiple_of(source * shard, shard), shard)],
            send_sem=cot_send.at[0],
            recv_sem=cot_recv.at[source],
            device_id=(g, source),
            device_id_type=MESH,
        ).wait_recv()

    def gating(row):
        for col in (x_left, x_right, x_opp):
            take_cot(row * LINE + col)

        @pl.when(row != z)
        def _():
            take_cot(row * LINE + x)

        def part(m, carry):
            at = pl.ds(pl.multiple_of(row * chunk + m * tall, tall), tall)
            acc[...] = jnp.dot(tok[at, :], wts[...], preferred_element_type=jnp.float32)
            gate = acc[:, :units] * scale
            up = acc[:, units:] * scale
            sigma = jax.nn.sigmoid(gate)
            upstream = cot[at, :].astype(jnp.float32)
            rows[at, :units] = (upstream * up * sigma * (1.0 + gate * (1.0 - sigma))).astype(jnp.bfloat16)
            rows[at, units:] = (upstream * gate * sigma).astype(jnp.bfloat16)
            return carry

        lax.fori_loop(0, chunk // tall, part, 0)

    def gradient(b):
        to = pl.ds(pl.multiple_of(b * tall, tall), tall)
        return lax.dot_general(
            tok[:, to], rows[...], (((0,), (0,)), ((), ())), preferred_element_type=jnp.float32
        )

    def finish_row(row):
        for p, q in zip(near, back):
            x_copy(row, x_left, q, 0).wait_recv()
            x_copy(row, x_right, p, 1).wait_recv()
            far_copy(row, x_opp, p, 0).wait_recv()
            far_copy(row, x_opp, q, 1).wait_recv()
        gating(row)

    def my_turn(i):
        pl.semaphore_signal(turn.at[i], inc=1, device_id=(twin, d), device_id_type=MESH)

    def wait_turn(i):
        pl.semaphore_wait(turn.at[i], 1)

    @pl.when(odd)
    def _():
        if OUTER_ODD == 0:
            exchange_outer()
        if TURN_Z >= 0:
            wait_turn(0)

    for p in range(PIECES):
        send_z(z, p)

    @pl.when(even)
    def _():
        for p in range(PIECES):
            send_x(z, p)

    @pl.when(even)
    def _():
        if TURN_Z == 0:
            my_turn(0)

    if INNER_AT == 0:
        exchange_inner()

    for k in range(1, LINE):
        row = row_of(k)
        for p in range(PIECES):
            take_z(row, p)

            @pl.when(even)
            def _():
                send_x(row, p)

        @pl.when(even)
        def _():
            if k == TURN_Z:
                my_turn(0)
            relay_x(row_of(k - 1))

        if k == INNER_AT:
            exchange_inner()
        if k == OUTER_AT and k == OUTER_ODD:
            exchange_outer()
        elif k == OUTER_AT:
            pl.when(even)(exchange_outer)
        elif k == OUTER_ODD:
            pl.when(odd)(exchange_outer)

    for load in loads[1:4]:
        load.wait()

    @pl.when(odd)
    def _():
        wait_turn(1)
        for k in range(LINE):
            for p in range(PIECES):
                send_x(row_of(k), p)
        for k in range(LINE - 1):
            relay_x(row_of(k))

    def all_rows(k, carry):
        finish_row(row_of(k))
        return carry

    lax.fori_loop(0, EARLY_ROWS, all_rows, 0)
    relay_x(row_of(LINE - 1))

    @pl.when(even)
    def _():
        my_turn(1)

    lax.fori_loop(EARLY_ROWS, LINE, all_rows, 0)

    def step_copy(b, way):
        to = pl.ds(pl.multiple_of(b * tall, tall), tall)
        return pltpu.make_async_remote_copy(
            src_ref=step.at[to],
            dst_ref=(from_twin if way == 0 else from_far).at[to],
            send_sem=step_send.at[way, b],
            recv_sem=step_recv.at[way, b],
            device_id=((twin if way == 0 else far), d),
            device_id_type=MESH,
        )

    def send_step(b):
        step_copy(b, 1).start()
        step_copy(b, 0).start()

    def final(b, carry):
        to = pl.ds(pl.multiple_of(b * tall, tall), tall)
        moved = wts[to, :].astype(jnp.float32) - 0.5 * (gradient(b) * scale)
        step[to, :] = moved.astype(jnp.bfloat16)

        @pl.when(b > 0)
        def _():
            send_step(b - 1)

        return carry

    lax.fori_loop(0, blocks, final, 0)
    send_step(blocks - 1)

    def sent_rows(k, carry):
        row = row_of(k)

        for p in range(PIECES):
            @pl.when((z < LINE - 1) & (row <= z))
            def _():
                z_copy(row, p, 0, z + 1).wait_send()

            @pl.when((z > 0) & (row >= z))
            def _():
                z_copy(row, p, 1, z - 1).wait_send()

            x_copy(row, x, p, 0).wait_send()
            x_copy(row, x, p, 1).wait_send()

        for p, q in zip(near, back):
            far_copy(row, x_left, p, 0).wait_send()
            far_copy(row, x_right, q, 1).wait_send()

        return carry

    lax.fori_loop(0, LINE, sent_rows, 0)

    def sent_cot(i, carry):
        cot_copy((d + i) % 16).wait_send()
        return carry

    lax.fori_loop(1, 16, sent_cot, 0)

    def out_copies(b):
        to = pl.ds(pl.multiple_of(b * tall, tall), tall)
        return (pltpu.make_async_copy(from_far.at[to], out.at[0, to], out_sem.at[b]),)

    def mix(b, carry):
        to = pl.ds(pl.multiple_of(b * tall, tall), tall)
        step_copy(b, 0).wait_recv()
        step_copy(b, 1).wait_recv()
        mixed = 0.5 * step[to, :].astype(jnp.float32) + 0.25 * (
            from_twin[to, :].astype(jnp.float32) + from_far[to, :].astype(jnp.float32)
        )
        from_far[to, :] = mixed.astype(jnp.bfloat16)

        @pl.when(b > 0)
        def _():
            for copy in out_copies(b - 1):
                copy.start()

        return carry

    lax.fori_loop(0, blocks, mix, 0)
    for copy in out_copies(blocks - 1):
        copy.start()

    def sent_blocks(b, carry):
        step_copy(b, 0).wait_send()
        step_copy(b, 1).wait_send()
        for copy in out_copies(b):
            copy.wait()
        return carry

    lax.fori_loop(0, blocks, sent_blocks, 0)


def split(mixed, out_gate, out_up, held, in_sem, out_sem):
    units = out_gate.shape[2]
    blocks = in_sem.shape[0]
    tall = held.shape[0] // blocks

    def take(b):
        at = pl.ds(b * tall, tall)
        return pltpu.make_async_copy(mixed.at[0, at], held.at[at], in_sem.at[b])

    def give(b):
        at = pl.ds(b * tall, tall)
        return (
            pltpu.make_async_copy(held.at[at, pl.ds(0, units)], out_gate.at[0, at], out_sem.at[0, b]),
            pltpu.make_async_copy(held.at[at, pl.ds(units, units)], out_up.at[0, at], out_sem.at[1, b]),
        )

    for b in range(blocks):
        take(b).start()
    for b in range(blocks):
        take(b).wait()
        for copy in give(b):
            copy.start()
    for b in range(blocks):
        for copy in give(b):
            copy.wait()


def solution(mesh):
    groups = mesh.shape["grp"]

    def local(tokens, hidden_grad, w_gate, w_up):
        shard, width = tokens.shape[1:]
        units = w_gate.shape[2]
        count = shard * mesh.shape["dp"]
        tall = 256
        blocks = width // tall
        dma = pltpu.SemaphoreType.DMA
        wide = 2 * units
        mixed = pl.pallas_call(
            functools.partial(kernel, groups),
            out_shape=jax.ShapeDtypeStruct((1, width, wide), jnp.bfloat16),
            in_specs=[pl.BlockSpec(memory_space=pl.ANY)] * 4,
            out_specs=pl.BlockSpec(memory_space=pl.ANY),
            scratch_shapes=[
                pltpu.VMEM((count, width), jnp.bfloat16),
                pltpu.VMEM((count, units), jnp.bfloat16),
                pltpu.VMEM(hidden_grad.shape[1:], jnp.bfloat16),
                pltpu.VMEM((width, wide), jnp.bfloat16),
                pltpu.VMEM((count, wide), jnp.bfloat16),
                pltpu.VMEM((tall, wide), jnp.float32),
                pltpu.VMEM((width, wide), jnp.bfloat16),
                pltpu.VMEM((width, wide), jnp.bfloat16),
                pltpu.VMEM((width, wide), jnp.bfloat16),
                dma((4,)),
                dma(()),
                dma((2, LINE, PIECES)),
                dma((LINE, PIECES)),
                dma((2, LINE, PIECES)),
                dma((2, LINE, PIECES)),
                dma((2, LINE, PIECES)),
                dma((2, LINE, PIECES)),
                dma((16,)),
                dma((16,)),
                dma((2, blocks)),
                dma((2, blocks)),
                dma((blocks,)),
                pltpu.SemaphoreType.REGULAR((2,)),
            ],
            compiler_params=pltpu.CompilerParams(
                collective_id=0, has_side_effects=True, vmem_limit_bytes=60 * 1024 * 1024
            ),
        )(tokens, hidden_grad, w_gate, w_up)
        out = jax.ShapeDtypeStruct(w_gate.shape, jnp.bfloat16)
        return pl.pallas_call(
            split,
            out_shape=(out, out),
            in_specs=[pl.BlockSpec(memory_space=pl.ANY)],
            out_specs=(pl.BlockSpec(memory_space=pl.ANY),) * 2,
            scratch_shapes=[pltpu.VMEM((width, wide), jnp.bfloat16), dma((4,)), dma((2, 4))],
            compiler_params=pltpu.CompilerParams(vmem_limit_bytes=60 * 1024 * 1024),
        )(mixed)

    in_specs = (
        P("grp", "dp", None),
        P("grp", "dp", None),
        P("grp", None, "dp"),
        P("grp", None, "dp"),
    )
    out_specs = (P("grp", None, "dp"), P("grp", None, "dp"))
    return jax.shard_map(local, mesh=mesh, in_specs=in_specs, out_specs=out_specs, check_vma=False)
```
